32 devices in a mesh: minor: 4 (over z), major: 8 (over y, x, core).
Axes of the slice: x: 2, y: 2, z: 4, core: 2. Of those that a mesh axis runs over, the one named last changes fastest.
Arguments:
- queries: bfloat16 [16384, 1024], P(('major', 'minor')), may hold values from -1.75 to 1.75
- keys: bfloat16 [16384, 1024], P(('major', 'minor')), may hold values from -1.75 to 1.75
- values: bfloat16 [16384, 1024], P(('major', 'minor')), may hold values from -1.75 to 1.75
- cotangent: bfloat16 [16384, 1024], P(('major', 'minor')), may hold values from -1.75 to 1.75
Outputs:
- attended: bfloat16 [16384, 1024], P(('major', 'minor'))
- grad_queries: bfloat16 [16384, 1024], P(('major', 'minor'))
- grad_keys: bfloat16 [16384, 1024], P(('major', 'minor'))
- grad_values: bfloat16 [16384, 1024], P(('major', 'minor'))
The draws below stay inside these ranges and needn't reach their ends.
All inputs are finite; a program needn't handle non-finite values.
Results may differ from the reference program's by a relative error of at most 0.0057.
Values sent between devices are 32-bit elements; how exact they have to be, the bound alone decides.
No kernel may reach another device: no remote copies, remote signals or barrier semaphores. Data moves between devices by JAX's collectives and lax.ppermute only.
A program may use at most 128 MiB of HBM per device.

```python
import jax
import jax.numpy as jnp
from jax import lax

H = 16
HD = 64
TOK_DEV = 512
TOKENS = 16384


def shard_levels(own_key, extent, pieces, least, top_value):
    loudness = 1.0
    for dim, shards_of in pieces:
        draws = jax.random.uniform(jax.random.fold_in(jax.random.fold_in(own_key, 6), dim), (shards_of,), jnp.float32, least / len(pieces), top_value / len(pieces))
        loudness = loudness * jnp.repeat(jnp.exp(draws), extent[dim] // shards_of).reshape((-1,) + (1,) * (len(extent) - 1 - dim))
    return loudness


def scatter_about(key, extent, deviation, limit, cuts=(), kind=jnp.bfloat16):
    values = deviation * jax.random.normal(key, extent, jnp.float32)
    if cuts:
        values = values * shard_levels(key, extent, cuts, -0.22, 0.18)
    return jnp.clip(values, -limit, limit).astype(kind)


def setup_inputs(seed: int = 0) -> dict:
    key_of = jax.random.split(jax.random.key(seed), 5)
    queries = scatter_about(key_of[0], (TOKENS, H * HD), 0.3, 1.75, ((0, 32),))
    keys = scatter_about(key_of[1], (TOKENS, H * HD), 0.3, 1.75, ((0, 32),))
    values = scatter_about(key_of[2], (TOKENS, H * HD), 0.3, 1.75, ((0, 32),))
    cotangent = scatter_about(key_of[3], (TOKENS, H * HD), 0.3, 1.75, ((0, 32),))
    return dict(queries=queries, keys=keys, values=values, cotangent=cotangent)


def block_terms(qb, kb, vb, gb, s_in, r_in, pos):
    rows = qb.shape[0]
    scale = 1.0 / jnp.sqrt(pos + 1.0)
    qf = qb.reshape(rows, H, HD).astype(jnp.float32)
    kf = kb.reshape(rows, H, HD).astype(jnp.float32)
    vf = vb.reshape(rows, H, HD).astype(jnp.float32)
    gf = gb.reshape(rows, H, HD).astype(jnp.float32)
    mask = (jnp.arange(rows)[:, None] >= jnp.arange(rows)[None, :])[None]
    scores = jnp.einsum('thd,shd->hts', qf, kf)
    weights = jnp.where(mask, scores * scale[None, :, None], 0.0).astype(jnp.bfloat16).astype(jnp.float32)
    backs = jnp.einsum('thd,shd->hts', gf, vf)
    back = jnp.where(mask, backs * scale[None, :, None], 0.0).astype(jnp.bfloat16).astype(jnp.float32)
    s_b = s_in.astype(jnp.bfloat16).astype(jnp.float32)
    r_b = r_in.astype(jnp.bfloat16).astype(jnp.float32)
    attended = jnp.einsum('hts,shd->thd', weights, vf) + scale[:, None, None] * jnp.einsum('thi,hij->thj', qf, s_b)
    grad_q = jnp.einsum('hts,shd->thd', back, kf) + scale[:, None, None] * jnp.einsum('thj,hij->thi', gf, s_b)
    grad_k = jnp.einsum('hts,thd->shd', back, qf) + jnp.einsum('shj,hij->shi', vf, r_b)
    grad_v = jnp.einsum('hts,thd->shd', weights, gf) + jnp.einsum('shi,hij->shj', kf, r_b)
    shaped = [x.reshape(rows, H * HD).astype(jnp.bfloat16) for x in (attended, grad_q, grad_k, grad_v)]
    return tuple(shaped)

def local_states(qb, kb, vb, gb, pos):
    rows = qb.shape[0]
    scale = 1.0 / jnp.sqrt(pos + 1.0)
    qf = qb.reshape(rows, H, HD).astype(jnp.float32)
    kf = kb.reshape(rows, H, HD).astype(jnp.float32)
    vf = vb.reshape(rows, H, HD).astype(jnp.float32)
    gf = gb.reshape(rows, H, HD).astype(jnp.float32)
    qc = (qf * scale[:, None, None]).astype(jnp.bfloat16).astype(jnp.float32)
    state = jnp.einsum('thi,thj->hij', kf, vf)
    adjoint = jnp.einsum('thi,thj->hij', qc, gf)
    return (state, adjoint)

def reference(queries, keys, values, cotangent):
    blocks = TOKENS // TOK_DEV
    split = lambda a: a.reshape(blocks, TOK_DEV, H * HD)
    qs, ks, vs, gs = (split(queries), split(keys), split(values), split(cotangent))
    starts = jnp.arange(blocks, dtype=jnp.int32)

    def position(index):
        return (index * TOK_DEV + jnp.arange(TOK_DEV, dtype=jnp.int32)).astype(jnp.float32)

    def states_of(item):
        qb, kb, vb, gb, index = item
        return local_states(qb, kb, vb, gb, position(index))
    s_all, r_all = lax.map(states_of, (qs, ks, vs, gs, starts))
    zero = jnp.zeros((H, HD, HD), jnp.float32)

    def accumulate(carry, term):
        return (carry + term, carry)
    _, s_in = lax.scan(accumulate, zero, s_all)
    _, r_in = lax.scan(accumulate, zero, r_all, reverse=True)

    def outputs_of(item):
        qb, kb, vb, gb, s_b, r_b, index = item
        return block_terms(qb, kb, vb, gb, s_b, r_b, position(index))
    results = lax.map(outputs_of, (qs, ks, vs, gs, s_in, r_in, starts))
    merged = [x.reshape(TOKENS, H * HD) for x in results]
    return (merged[0], merged[1], merged[2], merged[3])
```

```python
import functools

import jax
import jax.numpy as jnp
from jax import lax
from jax.experimental import pallas as pl
from jax.experimental.pallas import tpu as pltpu
from jax.sharding import PartitionSpec as P

HD = 64
LANES = 2 * HD
F32 = jnp.float32
BF16 = jnp.bfloat16


VM = pl.BlockSpec(memory_space=pltpu.VMEM)
ANY = pl.BlockSpec(memory_space=pltpu.HBM)


def dot(a, b, dims):
    return lax.dot_general(a, b, (dims, ((), ())), preferred_element_type=F32)


def nn(a, b):
    return dot(a, b, ((1,), (0,)))


def nt(a, b):
    return dot(a, b, ((1,), (1,)))


def tn(a, b):
    return dot(a, b, ((0,), (0,)))


def first_head(shape):
    return lax.broadcasted_iota(jnp.int32, shape, len(shape) - 1) < HD


def stacked(x):
    first = first_head(x.shape)
    zero = jnp.zeros_like(x)
    return jnp.concatenate([jnp.where(first, x, zero), jnp.where(first, zero, x)], 0)


def packed(m):
    return jnp.where(first_head((HD, LANES)), m[:HD], m[HD:])


def states_kernel(nz, q_hbm, k_hbm, v_hbm, g_hbm, q, k, v, g, qc, c, early, late, *rest):
    pieces, sem = rest[:nz], rest[nz]
    pairs, rows, _ = q.shape
    per = pairs // nz
    z = lax.axis_index("minor")
    block = lax.axis_index("major") * nz + z
    order = [(slot, i) for slot in range(nz - 1, -1, -1) for i in range(per)]

    def pair_of(slot, i):
        return jnp.bitwise_xor(z, slot) * per + i

    copies = []
    for n, (slot, i) in enumerate(order):
        p = pair_of(slot, i)
        lanes = pl.ds(pl.multiple_of(p * LANES, LANES), LANES)
        copies.append([
            pltpu.make_async_copy(src.at[:, lanes], dst.at[p], sem.at[a, n])
            for a, (src, dst) in enumerate(((k_hbm, k), (v_hbm, v), (q_hbm, q), (g_hbm, g)))
        ])
        for copy in copies[-1]:
            copy.start()
    pos = block * rows + lax.broadcasted_iota(jnp.int32, (rows, LANES), 0)
    c[...] = 1.0 / jnp.sqrt(pos.astype(F32) + 1.0)
    half = rows // 2
    for n, (slot, i) in enumerate(order):
        p = pair_of(slot, i)
        for copy in copies[n]:
            copy.wait()
        s_a = packed(tn(k[p, :half], v[p, :half]))
        s_b = packed(tn(k[p, half:], v[p, half:]))
        qc[p] = (q[p].astype(F32) * c[...]).astype(BF16)
        r_a = packed(tn(qc[p, :half], g[p, :half]))
        r_b = packed(tn(qc[p, half:], g[p, half:]))
        early[p] = s_a
        late[p] = r_b
        pieces[slot][i, 0] = s_a + s_b
        pieces[slot][i, 1] = r_a + r_b


def inner_kernel(first, count, q, k, v, g, qc, early, late, o_att, o_gq, o_gk, o_gv):
    rows = q.shape[1]
    half = rows // 2
    n = 128
    row = lax.broadcasted_iota(jnp.int32, (n, 2 * n), 0)
    col = jnp.bitwise_and(lax.broadcasted_iota(jnp.int32, (n, 2 * n), 1), n - 1)
    lower = row >= col
    upper = row <= col

    def one(step, carry):
        p = first + step
        s_bd = stacked(early[p].astype(BF16))
        r_bd = stacked(late[p].astype(BF16))
        chunk = lambda ref, i: ref[p, i * n:(i + 1) * n]
        per_half = half // n
        for h in range(2):
            for i in range(h * per_half, (h + 1) * per_half):
                at = slice(i * n, (i + 1) * n)
                att = gq = gk = gv = None
                if h == 1:
                    att = nn(chunk(q, i), s_bd)
                    gq = nt(chunk(g, i), s_bd)
                else:
                    gk = nt(chunk(v, i), r_bd)
                    gv = nn(chunk(k, i), r_bd)
                add = lambda total, x: x if total is None else total + x
                for j in range(h * per_half, i + 1):
                    ks, vs = stacked(chunk(k, j)), stacked(chunk(v, j))
                    w = nt(chunk(q, i), ks)
                    b = nt(chunk(g, i), vs)
                    if i == j:
                        w = jnp.where(lower, w, 0.0)
                        b = jnp.where(lower, b, 0.0)
                    att = add(att, nn(w.astype(BF16), vs))
                    gq = add(gq, nn(b.astype(BF16), ks))
                for j in range(i, (h + 1) * per_half):
                    gs, qs = stacked(chunk(g, j)), stacked(chunk(qc, j))
                    w = nt(chunk(k, i), qs)
                    b = nt(chunk(v, i), gs)
                    if i == j:
                        w = jnp.where(upper, w, 0.0)
                        b = jnp.where(upper, b, 0.0)
                    gv = add(gv, nn(w.astype(BF16), gs))
                    gk = add(gk, nn(b.astype(BF16), qs))
                o_att[step, at] = att
                o_gq[step, at] = gq
                o_gk[step, at] = gk
                o_gv[step, at] = gv
        return carry

    lax.fori_loop(0, count, one, 0)


def totals_kernel(nz, *refs):
    total = refs[0][...]
    for s in range(1, nz):
        total = total + refs[s][...]
    refs[nz][...] = total


def column_kernel(t, t_other, out):
    core = jnp.bitwise_and(lax.axis_index("major"), 1)
    n = HD // 2
    at = pl.ds(pl.multiple_of(core * n, n), n)
    out[...] = t[:, :, at] + t_other[:, :, at]


def offsets_kernel(masks, *refs):
    out = refs[-1]
    major = lax.axis_index("major")
    s = r = jnp.zeros_like(out[:, 0])
    for ref, mask in zip(refs, masks):
        peer = jnp.bitwise_xor(major, mask)
        s = s + jnp.where(peer < major, ref[:, 0], 0.0)
        r = r + jnp.where(peer > major, ref[:, 1], 0.0)
    out[:, 0] = s
    out[:, 1] = r


def prefixes_kernel(nz, *refs):
    raw, (t_other, x_own, x_other), out = refs[:nz], refs[nz:nz + 3], refs[nz + 3:]
    core = jnp.bitwise_and(lax.axis_index("major"), 1)
    z = lax.axis_index("minor")
    n = HD // 2
    for kind in range(2):
        lo = jnp.where(core == 0, x_own[:, kind], x_other[:, kind])
        hi = jnp.where(core == 0, x_other[:, kind], x_own[:, kind])
        base = jnp.concatenate([lo, hi], 1)
        base = base + jnp.where(core == 1 - kind, t_other[:, kind], 0.0)
        for slot in range(nz):
            there = jnp.bitwise_xor(z, slot)
            total = base
            for s in range(nz):
                if s == slot:
                    continue
                source = jnp.bitwise_xor(z, s)
                counts = source < there if kind == 0 else source > there
                total = total + jnp.where(counts, raw[s][:, kind], 0.0)
            out[slot][:, kind] = total


def outer_kernel(nz, parts, *refs):
    q, k, v, g, c = refs[:5]
    inner = refs[5:5 + 4 * parts]
    pieces = refs[5 + 4 * parts:5 + 4 * parts + nz]
    outs = refs[5 + 4 * parts + nz:9 + 4 * parts + nz]
    stage, sem = refs[9 + 4 * parts + nz:]
    pairs, rows, _ = q.shape
    per = pairs // nz
    z = lax.axis_index("minor")
    copies = []
    for slot in range(nz):
        for i in range(per):
            n = slot * per + i
            p = jnp.bitwise_xor(z, slot) * per + i
            s_bd = stacked(pieces[slot][i, 0].astype(BF16))
            r_bd = stacked(pieces[slot][i, 1].astype(BF16))
            scale = c[...]
            results = (
                (inner[0][p] + nn(q[p], s_bd)) * scale,
                (inner[1][p] + nt(g[p], s_bd)) * scale,
                inner[2][p] + nt(v[p], r_bd),
                inner[3][p] + nn(k[p], r_bd),
            )
            lanes = pl.ds(pl.multiple_of(p * LANES, LANES), LANES)
            for a, result in enumerate(results):
                stage[a, n] = result.astype(BF16)
                copy = pltpu.make_async_copy(stage.at[a, n], outs[a].at[:, lanes], sem.at[a, n])
                copy.start()
                copies.append(copy)
    for copy in copies:
        copy.wait()


def call(body, outs, ins, n_hbm=0, out_hbm=False, scratch=(), mib=8, flops=0, name=None):
    return pl.pallas_call(
        body,
        out_shape=outs if out_hbm else tuple(pltpu.VMEM(s, d) for s, d in outs),
        in_specs=[ANY] * n_hbm + [VM] * (len(ins) - n_hbm),
        out_specs=tuple((ANY if out_hbm else VM) for _ in outs),
        scratch_shapes=scratch,
        compiler_params=pltpu.CompilerParams(vmem_limit_bytes=mib * 2**20),
        cost_estimate=pl.CostEstimate(flops=flops, transcendentals=0, bytes_accessed=0),
        name=name,
    )(*ins)


def swap(x, axis, count, mask):
    return lax.ppermute(x, axis, [(i, i ^ mask) for i in range(count)])


def on_device(queries, keys, values, cotangent):
    rows, columns = queries.shape
    pairs = columns // LANES
    nz, nm = lax.axis_size("minor"), lax.axis_size("major")
    per = pairs // nz
    plane = ((pairs, rows, LANES), BF16)
    piece = ((per, 2, HD, LANES), F32)
    half_piece = ((per, 2, HD // 2, LANES), F32)
    state = ((pairs, HD, LANES), F32)
    q, k, v, g, qc, c, early, late, *mine = call(
        functools.partial(states_kernel, nz),
        [plane] * 5 + [((rows, LANES), F32), state, state] + [piece] * nz,
        (queries, keys, values, cotangent),
        n_hbm=4,
        scratch=[pltpu.SemaphoreType.DMA((4, pairs))],
        name="states",
    )
    raw = [mine[0]] + [None] * (nz - 1)
    for s in range(nz - 1, 0, -1):
        raw[s] = swap(mine[s], "minor", nz, s)

    inner = call(
        functools.partial(inner_kernel, 0, pairs),
        [((pairs, rows, LANES), F32)] * 4,
        (q, k, v, g, qc, early, late),
        flops=10**9,
        name="inner",
    )

    (total,) = call(functools.partial(totals_kernel, nz), [piece], raw, name="totals")
    t_other = swap(total, "major", nm, 1)
    (col,) = call(column_kernel, [half_piece], (total, t_other), name="column")
    masks = list(range(2, nm, 2))
    peers = [swap(col, "major", nm, m) for m in masks]
    (x_own,) = call(functools.partial(offsets_kernel, masks), [half_piece], peers, name="offsets")
    x_other = swap(x_own, "major", nm, 1)
    ready = call(
        functools.partial(prefixes_kernel, nz), [piece] * nz, (*raw, t_other, x_own, x_other),
        name="prefixes",
    )
    states = [ready[0]] + [None] * (nz - 1)
    for s in range(nz - 1, 0, -1):
        states[s] = swap(ready[s], "minor", nz, s)

    out = jax.ShapeDtypeStruct((rows, columns), BF16)
    return call(
        functools.partial(outer_kernel, nz, 1),
        (out,) * 4,
        (q, k, v, g, c, *inner, *states),
        out_hbm=True,
        scratch=[pltpu.VMEM((4, pairs, rows, LANES), BF16), pltpu.SemaphoreType.DMA((4, pairs))],
        mib=12,
        flops=10**8,
        name="outer",
    )


def solution(mesh):
    spec = P(("major", "minor"), None)
    return jax.shard_map(
        on_device, mesh=mesh, in_specs=(spec,) * 4, out_specs=(spec,) * 4, check_vma=False
    )
```

```python
import functools

import jax
import jax.numpy as jnp
from jax import lax
from jax.experimental import pallas as pl
from jax.experimental.pallas import tpu as pltpu
from jax.sharding import PartitionSpec as P

HD = 64
LANES = 2 * HD
F32 = jnp.float32
BF16 = jnp.bfloat16


VM = pl.BlockSpec(memory_space=pltpu.VMEM)
ANY = pl.BlockSpec(memory_space=pltpu.HBM)


def dot(a, b, dims):
    return lax.dot_general(a, b, (dims, ((), ())), preferred_element_type=F32)


def nn(a, b):
    return dot(a, b, ((1,), (0,)))


def nt(a, b):
    return dot(a, b, ((1,), (1,)))


def tn(a, b):
    return dot(a, b, ((0,), (0,)))


def first_head(shape):
    return lax.broadcasted_iota(jnp.int32, shape, len(shape) - 1) < HD


def stacked(x):
    first = first_head(x.shape)
    zero = jnp.zeros_like(x)
    return jnp.concatenate([jnp.where(first, x, zero), jnp.where(first, zero, x)], 0)


def packed(m):
    return jnp.where(first_head((HD, LANES)), m[:HD], m[HD:])


def states_kernel(nz, q_hbm, k_hbm, v_hbm, g_hbm, q, k, v, g, qc, c, early, late, *rest):
    pieces, sem = rest[:nz], rest[nz]
    pairs, rows, _ = q.shape
    per = pairs // nz
    z = lax.axis_index("minor")
    block = lax.axis_index("major") * nz + z
    order = [(slot, i) for slot in range(nz - 1, -1, -1) for i in range(per)]

    def pair_of(slot, i):
        return jnp.bitwise_xor(z, slot) * per + i

    copies = []
    for n, (slot, i) in enumerate(order):
        p = pair_of(slot, i)
        lanes = pl.ds(pl.multiple_of(p * LANES, LANES), LANES)
        copies.append([
            pltpu.make_async_copy(src.at[:, lanes], dst.at[slot * per + i], sem.at[a, n])
            for a, (src, dst) in enumerate(((k_hbm, k), (v_hbm, v), (q_hbm, q), (g_hbm, g)))
        ])
        for copy in copies[-1]:
            copy.start()
    pos = block * rows + lax.broadcasted_iota(jnp.int32, (rows, LANES), 0)
    c[...] = 1.0 / jnp.sqrt(pos.astype(F32) + 1.0)
    half = rows // 2
    for n, (slot, i) in enumerate(order):
        p = slot * per + i
        for copy in copies[n]:
            copy.wait()
        s_a = packed(tn(k[p, :half], v[p, :half]))
        s_b = packed(tn(k[p, half:], v[p, half:]))
        qc[p] = (q[p].astype(F32) * c[...]).astype(BF16)
        r_a = packed(tn(qc[p, :half], g[p, :half]))
        r_b = packed(tn(qc[p, half:], g[p, half:]))
        early[p] = s_a
        late[p] = r_b
        pieces[slot][i, 0] = s_a + s_b
        pieces[slot][i, 1] = r_a + r_b


def inner_kernel(first, count, q, k, v, g, qc, early, late, *rest):
    o_att, o_gq, o_gk, o_gv = rest[-4:]
    rows = q.shape[1]
    half = rows // 2
    n = 128
    row = lax.broadcasted_iota(jnp.int32, (n, 2 * n), 0)
    col = jnp.bitwise_and(lax.broadcasted_iota(jnp.int32, (n, 2 * n), 1), n - 1)
    lower = row >= col
    upper = row <= col

    def one(step, carry):
        p = first + step
        s_bd = stacked(early[p].astype(BF16))
        r_bd = stacked(late[p].astype(BF16))
        chunk = lambda ref, i: ref[p, i * n:(i + 1) * n]
        per_half = half // n
        for h in range(2):
            for i in range(h * per_half, (h + 1) * per_half):
                at = slice(i * n, (i + 1) * n)
                att = gq = gk = gv = None
                if h == 1:
                    att = nn(chunk(q, i), s_bd)
                    gq = nt(chunk(g, i), s_bd)
                else:
                    gk = nt(chunk(v, i), r_bd)
                    gv = nn(chunk(k, i), r_bd)
                add = lambda total, x: x if total is None else total + x
                for j in range(h * per_half, i + 1):
                    ks, vs = stacked(chunk(k, j)), stacked(chunk(v, j))
                    w = nt(chunk(q, i), ks)
                    b = nt(chunk(g, i), vs)
                    if i == j:
                        w = jnp.where(lower, w, 0.0)
                        b = jnp.where(lower, b, 0.0)
                    att = add(att, nn(w.astype(BF16), vs))
                    gq = add(gq, nn(b.astype(BF16), ks))
                for j in range(i, (h + 1) * per_half):
                    gs, qs = stacked(chunk(g, j)), stacked(chunk(qc, j))
                    w = nt(chunk(k, i), qs)
                    b = nt(chunk(v, i), gs)
                    if i == j:
                        w = jnp.where(upper, w, 0.0)
                        b = jnp.where(upper, b, 0.0)
                    gv = add(gv, nn(w.astype(BF16), gs))
                    gk = add(gk, nn(b.astype(BF16), qs))
                o_att[step, at] = att
                o_gq[step, at] = gq
                o_gk[step, at] = gk
                o_gv[step, at] = gv
        return carry

    lax.fori_loop(0, count, one, 0)


def totals_kernel(nz, *refs):
    total = refs[0][...]
    for s in range(1, nz):
        total = total + refs[s][...]
    refs[-1][...] = total


def column_kernel(t, t_other, out):
    core = jnp.bitwise_and(lax.axis_index("major"), 1)
    n = HD // 2
    at = pl.ds(pl.multiple_of(core * n, n), n)
    out[...] = t[:, :, at] + t_other[:, :, at]


def offsets_kernel(masks, *refs):
    out = refs[-1]
    major = lax.axis_index("major")
    s = r = jnp.zeros_like(out[:, 0])
    for ref, mask in zip(refs, masks):
        peer = jnp.bitwise_xor(major, mask)
        s = s + jnp.where(peer < major, ref[:, 0], 0.0)
        r = r + jnp.where(peer > major, ref[:, 1], 0.0)
    out[:, 0] = s
    out[:, 1] = r


def prefixes_kernel(nz, *refs):
    raw, (t_other, x_own, x_other), out = refs[:nz], refs[nz:nz + 3], refs[nz + 3:]
    core = jnp.bitwise_and(lax.axis_index("major"), 1)
    z = lax.axis_index("minor")
    n = HD // 2
    for kind in range(2):
        lo = jnp.where(core == 0, x_own[:, kind], x_other[:, kind])
        hi = jnp.where(core == 0, x_other[:, kind], x_own[:, kind])
        base = jnp.concatenate([lo, hi], 1)
        base = base + jnp.where(core == 1 - kind, t_other[:, kind], 0.0)
        for slot in range(nz):
            there = jnp.bitwise_xor(z, slot)
            total = base
            for s in range(nz):
                if s == slot:
                    continue
                source = jnp.bitwise_xor(z, s)
                counts = source < there if kind == 0 else source > there
                total = total + jnp.where(counts, raw[s][:, kind], 0.0)
            out[slot][:, kind] = total


def outer_kernel(nz, cuts, *refs):
    parts = len(cuts) - 1
    q, k, v, g, c = refs[:5]
    inner = refs[5:5 + 4 * parts]
    pieces = refs[5 + 4 * parts:5 + 4 * parts + nz]
    outs = refs[5 + 4 * parts + nz:9 + 4 * parts + nz]
    stage, sem = refs[9 + 4 * parts + nz:]
    pairs, rows, _ = q.shape
    per = pairs // nz
    z = lax.axis_index("minor")
    copies = []
    for slot in range(nz):
        for i in range(per):
            n = slot * per + i
            p = jnp.bitwise_xor(z, slot) * per + i
            s_bd = stacked(pieces[slot][i, 0].astype(BF16))
            r_bd = stacked(pieces[slot][i, 1].astype(BF16))
            scale = c[...]
            part = max(j for j in range(parts) if cuts[j] <= n)
            own = [ref[n - cuts[part]] for ref in inner[4 * part:4 * part + 4]]
            results = (
                (own[0] + nn(q[n], s_bd)) * scale,
                (own[1] + nt(g[n], s_bd)) * scale,
                own[2] + nt(v[n], r_bd),
                own[3] + nn(k[n], r_bd),
            )
            lanes = pl.ds(pl.multiple_of(p * LANES, LANES), LANES)
            for a, result in enumerate(results):
                stage[a, n] = result.astype(BF16)
                copy = pltpu.make_async_copy(stage.at[a, n], outs[a].at[:, lanes], sem.at[a, n])
                copy.start()
                copies.append(copy)
    for copy in copies:
        copy.wait()


def call(body, outs, ins, n_hbm=0, out_hbm=False, scratch=(), mib=8, flops=0, name=None):
    return pl.pallas_call(
        body,
        out_shape=outs if out_hbm else tuple(pltpu.VMEM(s, d) for s, d in outs),
        in_specs=[ANY] * n_hbm + [VM] * (len(ins) - n_hbm),
        out_specs=tuple((ANY if out_hbm else VM) for _ in outs),
        scratch_shapes=scratch,
        compiler_params=pltpu.CompilerParams(vmem_limit_bytes=mib * 2**20),
        cost_estimate=pl.CostEstimate(flops=flops, transcendentals=0, bytes_accessed=0),
        name=name,
    )(*ins)


def swap(x, axis, count, mask):
    return lax.ppermute(x, axis, [(i, i ^ mask) for i in range(count)])


def on_device(queries, keys, values, cotangent):
    rows, columns = queries.shape
    pairs = columns // LANES
    nz, nm = lax.axis_size("minor"), lax.axis_size("major")
    per = pairs // nz
    plane = ((pairs, rows, LANES), BF16)
    piece = ((per, 2, HD, LANES), F32)
    half_piece = ((per, 2, HD // 2, LANES), F32)
    state = ((pairs, HD, LANES), F32)
    q, k, v, g, qc, c, early, late, *mine = call(
        functools.partial(states_kernel, nz),
        [plane] * 5 + [((rows, LANES), F32), state, state] + [piece] * nz,
        [pltpu.with_memory_space_constraint(x, pltpu.HBM) for x in (queries, keys, values, cotangent)],
        n_hbm=4,
        scratch=[pltpu.SemaphoreType.DMA((4, pairs))],
        name="states",
    )
    raw = [mine[0]] + [None] * (nz - 1)
    for s in range(nz - 1, 0, -1):
        raw[s] = swap(mine[s], "minor", nz, s)

    cuts = [0, 5 * pairs // 8, pairs]
    inner = []

    def work(after):
        n = len(inner)
        first, count = cuts[n], cuts[n + 1] - cuts[n]
        inner.append(call(
            functools.partial(inner_kernel, first, count),
            [((count, rows, LANES), F32)] * 4,
            (q, k, v, g, qc, early, late, *after),
            flops=count * 10**9,
            name="inner",
        ))
        return (inner[-1][0],)

    tail = work(())
    (total,) = call(functools.partial(totals_kernel, nz), [piece], (*raw, *tail), name="totals")
    t_other = swap(total, "major", nm, 1)
    (col,) = call(column_kernel, [half_piece], (total, t_other), name="column")
    masks = list(range(2, nm, 2))
    peers = [swap(col, "major", nm, m) for m in masks]
    (x_own,) = call(functools.partial(offsets_kernel, masks), [half_piece], peers, name="offsets")
    x_other = swap(x_own, "major", nm, 1)
    ready = call(
        functools.partial(prefixes_kernel, nz), [piece] * nz, (*raw, t_other, x_own, x_other),
        name="prefixes",
    )
    work((ready[0],))
    states = [ready[0]] + [None] * (nz - 1)
    for s in range(nz - 1, 0, -1):
        states[s] = swap(ready[s], "minor", nz, s)

    out = jax.ShapeDtypeStruct((rows, columns), BF16)
    return call(
        functools.partial(outer_kernel, nz, cuts),
        (out,) * 4,
        (q, k, v, g, c, *[x for part in inner for x in part], *states),
        out_hbm=True,
        scratch=[pltpu.VMEM((4, pairs, rows, LANES), BF16), pltpu.SemaphoreType.DMA((4, pairs))],
        mib=12,
        flops=10**8,
        name="outer",
    )


def solution(mesh):
    spec = P(("major", "minor"), None)
    return jax.shard_map(
        on_device, mesh=mesh, in_specs=(spec,) * 4, out_specs=(spec,) * 4, check_vma=False
    )
```

```python
import functools

import jax
import jax.numpy as jnp
from jax import lax
from jax.experimental import pallas as pl
from jax.experimental.pallas import tpu as pltpu
from jax.sharding import PartitionSpec as P

HD = 64
LANES = 2 * HD
F32 = jnp.float32
BF16 = jnp.bfloat16
CUTS = (0, 2, 3, 4, 5, 6, 8)


VM = pl.BlockSpec(memory_space=pltpu.VMEM)
ANY = pl.BlockSpec(memory_space=pltpu.HBM)


def dot(a, b, dims):
    return lax.dot_general(a, b, (dims, ((), ())), preferred_element_type=F32)


def nn(a, b):
    return dot(a, b, ((1,), (0,)))


def nt(a, b):
    return dot(a, b, ((1,), (1,)))


def tn(a, b):
    return dot(a, b, ((0,), (0,)))


def first_head(shape):
    return lax.broadcasted_iota(jnp.int32, shape, len(shape) - 1) < HD


def stacked(x):
    first = first_head(x.shape)
    zero = jnp.zeros_like(x)
    return jnp.concatenate([jnp.where(first, x, zero), jnp.where(first, zero, x)], 0)


def packed(m):
    return jnp.where(first_head((HD, LANES)), m[:HD], m[HD:])


def fetch(nz, sources, planes, sem):
    per = planes[0].shape[0] // nz
    z = lax.axis_index("minor")
    order = [slot * per + i for slot in range(nz - 1, -1, -1) for i in range(per)]
    copies = {}
    for n in order:
        p = jnp.bitwise_xor(z, n // per) * per + n % per
        lanes = pl.ds(pl.multiple_of(p * LANES, LANES), LANES)
        copies[n] = [
            pltpu.make_async_copy(src.at[:, lanes], dst.at[n], sem.at[a, n])
            for a, (src, dst) in enumerate(zip(sources, planes))
        ]
        for copy in copies[n]:
            copy.start()
    return order, copies


def key_states_kernel(nz, k_hbm, v_hbm, k, v, early, *rest):
    pieces, sem = rest[:nz], rest[nz]
    order, copies = fetch(nz, (k_hbm, v_hbm), (k, v), sem)
    half = k.shape[1] // 2
    per = k.shape[0] // nz
    for n in order:
        for copy in copies[n]:
            copy.wait()
        s_a = packed(tn(k[n, :half], v[n, :half]))
        s_b = packed(tn(k[n, half:], v[n, half:]))
        early[n] = s_a
        pieces[n // per][n % per] = s_a + s_b


def query_states_kernel(nz, q_hbm, g_hbm, q, g, qc, c, late, *rest):
    pieces, sem = rest[:nz], rest[nz]
    order, copies = fetch(nz, (q_hbm, g_hbm), (q, g), sem)
    rows = q.shape[1]
    half = rows // 2
    per = q.shape[0] // nz
    block = lax.axis_index("major") * nz + lax.axis_index("minor")
    pos = block * rows + lax.broadcasted_iota(jnp.int32, (rows, LANES), 0)
    c[...] = 1.0 / jnp.sqrt(pos.astype(F32) + 1.0)
    for n in order:
        for copy in copies[n]:
            copy.wait()
        qc[n] = (q[n].astype(F32) * c[...]).astype(BF16)
        r_a = packed(tn(qc[n, :half], g[n, :half]))
        r_b = packed(tn(qc[n, half:], g[n, half:]))
        late[n] = r_b
        pieces[n // per][n % per] = r_a + r_b


def turned(w):
    n = w.shape[0]
    return jnp.concatenate([w[:, :n].T, w[:, n:].T], 1)


def inner_kernel(first, count, k, v, g, qc, early, late, o_att, o_gq, o_gk, o_gv):
    n = k.shape[1] // 2
    row = lax.broadcasted_iota(jnp.int32, (n, 2 * n), 0)
    col = jnp.bitwise_and(lax.broadcasted_iota(jnp.int32, (n, 2 * n), 1), n - 1)
    lower = row >= col
    for step in range(count):
        p = first + step
        s_bd = stacked(early[p].astype(BF16))
        r_bd = stacked(late[p].astype(BF16))
        for h in range(2):
            at = slice(h * n, (h + 1) * n)
            ks, vs, gs, qs = (stacked(ref[p, at]) for ref in (k, v, g, qc))
            w = jnp.where(lower, nt(qc[p, at], ks), 0.0).astype(BF16)
            b = jnp.where(lower, nt(g[p, at], vs), 0.0).astype(BF16)
            att = nn(w, vs)
            gq = nn(b, ks)
            gv = nn(turned(w), gs)
            gk = nn(turned(b), qs)
            if h == 1:
                att = att + nn(qc[p, at], s_bd)
                gq = gq + nt(g[p, at], s_bd)
            else:
                gk = gk + nt(v[p, at], r_bd)
                gv = gv + nn(k[p, at], r_bd)
            o_att[step, at] = att
            o_gq[step, at] = gq
            o_gk[step, at] = gk
            o_gv[step, at] = gv


def totals_kernel(nz, *refs):
    total = refs[0][...]
    for s in range(1, nz):
        total = total + refs[s][...]
    refs[nz][...] = total


def column_kernel(t, t_other, out):
    core = jnp.bitwise_and(lax.axis_index("major"), 1)
    n = HD // 2
    at = pl.ds(pl.multiple_of(core * n, n), n)
    out[...] = t[:, at] + t_other[:, at]


def offsets_kernel(kind, masks, *refs):
    out = refs[-1]
    major = lax.axis_index("major")
    total = jnp.zeros(out.shape, F32)
    for ref, mask in zip(refs, masks):
        peer = jnp.bitwise_xor(major, mask)
        counts = peer < major if kind == 0 else peer > major
        total = total + jnp.where(counts, ref[...], 0.0)
    out[...] = total


def prefixes_kernel(kind, nz, *refs):
    raw, (t_other, x_own, x_other), out = refs[:nz], refs[nz:nz + 3], refs[nz + 3:]
    core = jnp.bitwise_and(lax.axis_index("major"), 1)
    z = lax.axis_index("minor")
    lo = jnp.where(core == 0, x_own[...], x_other[...])
    hi = jnp.where(core == 0, x_other[...], x_own[...])
    base = jnp.concatenate([lo, hi], 1)
    base = base + jnp.where(core == 1 - kind, t_other[...], 0.0)
    for slot in range(nz):
        there = jnp.bitwise_xor(z, slot)
        total = base
        for s in range(nz):
            if s == slot:
                continue
            source = jnp.bitwise_xor(z, s)
            counts = source < there if kind == 0 else source > there
            total = total + jnp.where(counts, raw[s][...], 0.0)
        out[slot][...] = total


def outer_kernel(kind, nz, cuts, *refs):
    parts = len(cuts) - 1
    x, y, c = refs[:3]
    inner = refs[3:3 + 2 * parts]
    pieces = refs[3 + 2 * parts:3 + 2 * parts + nz]
    out_x, out_y, stage, sem = refs[3 + 2 * parts + nz:]
    per = x.shape[0] // nz
    z = lax.axis_index("minor")
    copies = []
    for n in range(x.shape[0]):
        slot, i = divmod(n, per)
        p = jnp.bitwise_xor(z, slot) * per + i
        lanes = pl.ds(pl.multiple_of(p * LANES, LANES), LANES)
        state = stacked(pieces[slot][i].astype(BF16))
        part = max(j for j in range(parts) if cuts[j] <= n)
        own = [ref[n - cuts[part]] for ref in inner[2 * part:2 * part + 2]]
        first = own[0] + nn(x[n], state)
        second = own[1] + nt(y[n], state)
        if kind == 0:
            second = second * c[...]
        for a, (result, out) in enumerate(((first, out_x), (second, out_y))):
            stage[a, n] = result.astype(BF16)
            copy = pltpu.make_async_copy(stage.at[a, n], out.at[:, lanes], sem.at[a, n])
            copy.start()
            copies.append(copy)
    for copy in copies:
        copy.wait()


class Chain:
    def __init__(self):
        self.after = ()

    def __call__(self, body, outs, ins, n_hbm=0, out_hbm=False, scratch=(), mib=8, flops=0, name=None):
        n_in, n_after = len(ins), len(self.after)

        def kernel(*refs):
            body(*refs[:n_in], *refs[n_in + n_after:])

        result = pl.pallas_call(
            kernel,
            out_shape=outs if out_hbm else tuple(pltpu.VMEM(s, d) for s, d in outs),
            in_specs=[ANY] * n_hbm + [VM] * (n_in - n_hbm) + [self.spec] * n_after if n_after
            else [ANY] * n_hbm + [VM] * (n_in - n_hbm),
            out_specs=tuple((ANY if out_hbm else VM) for _ in outs),
            scratch_shapes=scratch,
            compiler_params=pltpu.CompilerParams(vmem_limit_bytes=mib * 2**20),
            cost_estimate=pl.CostEstimate(flops=flops, transcendentals=0, bytes_accessed=0),
            name=name,
        )(*ins, *self.after)
        self.after = (result[0],)
        self.spec = ANY if out_hbm else VM
        return result


def swap(x, axis, count, mask):
    return lax.ppermute(x, axis, [(i, i ^ mask) for i in range(count)])


def spread(own, nz):
    out = [own[0]] + [None] * (nz - 1)
    for s in range(nz - 1, 0, -1):
        out[s] = swap(own[s], "minor", nz, s)
    return out


def on_device(queries, keys, values, cotangent):
    rows, columns = queries.shape
    pairs = columns // LANES
    nz, nm = lax.axis_size("minor"), lax.axis_size("major")
    per = pairs // nz
    plane = ((pairs, rows, LANES), BF16)
    piece = ((per, HD, LANES), F32)
    half_piece = ((per, HD // 2, LANES), F32)
    state = ((pairs, HD, LANES), F32)
    masks = list(range(2, nm, 2))
    run = Chain()
    hbm = lambda *xs: [pltpu.with_memory_space_constraint(x, pltpu.HBM) for x in xs]
    sems = [pltpu.SemaphoreType.DMA((2, pairs))]

    k, v, early, *mine_s = run(
        functools.partial(key_states_kernel, nz), [plane] * 2 + [state] + [piece] * nz,
        hbm(keys, values), n_hbm=2, scratch=sems, name="key_states",
    )
    raw_s = spread(mine_s, nz)
    q, g, qc, c, late, *mine_r = run(
        functools.partial(query_states_kernel, nz),
        [plane] * 3 + [((rows, LANES), F32), state] + [piece] * nz,
        hbm(queries, cotangent), n_hbm=2, scratch=sems, name="query_states",
    )
    raw_r = spread(mine_r, nz)

    cuts = [n * pairs // 8 for n in CUTS]
    inner = []

    def work():
        n = len(inner)
        first, count = cuts[n], cuts[n + 1] - cuts[n]
        inner.append(run(
            functools.partial(inner_kernel, first, count), [((count, rows, LANES), F32)] * 4,
            (k, v, g, qc, early, late), mib=16, flops=count * 5 * 10**8, name="inner",
        ))

    def totals(raw):
        (t,) = run(functools.partial(totals_kernel, nz), [piece], raw, name="totals")
        return t, swap(t, "major", nm, 1)

    def column(t):
        (col,) = run(column_kernel, [half_piece], t, name="column")
        return [swap(col, "major", nm, m) for m in masks]

    def offsets(kind, peers):
        (x,) = run(functools.partial(offsets_kernel, kind, masks), [half_piece], peers, name="offsets")
        return x, swap(x, "major", nm, 1)

    def prefixes(kind, raw, t, x):
        ready = run(
            functools.partial(prefixes_kernel, kind, nz), [piece] * nz, (*raw, t[1], *x),
            name="prefixes",
        )
        return spread(ready, nz)

    work()
    t_s = totals(raw_s)
    work()
    peers_s = column(t_s)
    work()
    x_s = offsets(0, peers_s)
    t_r = totals(raw_r)
    work()
    s_in = prefixes(0, raw_s, t_s, x_s)
    peers_r = column(t_r)
    work()
    x_r = offsets(1, peers_r)
    r_in = prefixes(1, raw_r, t_r, x_r)
    work()

    def outer(kind, x, y, which, pieces):
        parts = [part[a] for part in inner for a in which]
        out = jax.ShapeDtypeStruct((rows, columns), BF16)
        return run(
            functools.partial(outer_kernel, kind, nz, cuts), (out,) * 2,
            (x, y, c, *parts, *pieces), out_hbm=True,
            scratch=[pltpu.VMEM((2, pairs, rows, LANES), BF16), pltpu.SemaphoreType.DMA((2, pairs))],
            mib=12, flops=10**8, name="outer",
        )

    attended, grad_q = outer(0, qc, g, (0, 1), s_in)
    grad_v, grad_k = outer(1, k, v, (3, 2), r_in)
    return attended, grad_q, grad_k, grad_v


def solution(mesh):
    spec = P(("major", "minor"), None)
    return jax.shard_map(
        on_device, mesh=mesh, in_specs=(spec,) * 4, out_specs=(spec,) * 4, check_vma=False
    )
```

```python
import functools

import jax
import jax.numpy as jnp
from jax import lax
from jax.experimental import pallas as pl
from jax.experimental.pallas import tpu as pltpu
from jax.sharding import PartitionSpec as P

HD = 64
LANES = 2 * HD
F32 = jnp.float32
BF16 = jnp.bfloat16
CUTS = (0, 5, 8)


VM = pl.BlockSpec(memory_space=pltpu.VMEM)
ANY = pl.BlockSpec(memory_space=pltpu.HBM)


def dot(a, b, dims):
    return lax.dot_general(a, b, (dims, ((), ())), preferred_element_type=F32)


def nn(a, b):
    return dot(a, b, ((1,), (0,)))


def nt(a, b):
    return dot(a, b, ((1,), (1,)))


def tn(a, b):
    return dot(a, b, ((0,), (0,)))


def first_head(shape):
    return lax.broadcasted_iota(jnp.int32, shape, len(shape) - 1) < HD


def stacked(x):
    first = first_head(x.shape)
    zero = jnp.zeros_like(x)
    return jnp.concatenate([jnp.where(first, x, zero), jnp.where(first, zero, x)], 0)


def packed(m):
    return jnp.where(first_head((HD, LANES)), m[:HD], m[HD:])


def fetch(nz, sources, planes, sem):
    per = planes[0].shape[0] // nz
    z = lax.axis_index("minor")
    order = [slot * per + i for slot in range(nz - 1, -1, -1) for i in range(per)]
    copies = {}
    for n in order:
        p = jnp.bitwise_xor(z, n // per) * per + n % per
        lanes = pl.ds(pl.multiple_of(p * LANES, LANES), LANES)
        copies[n] = [
            pltpu.make_async_copy(src.at[:, lanes], dst.at[n], sem.at[a, n])
            for a, (src, dst) in enumerate(zip(sources, planes))
        ]
        for copy in copies[n]:
            copy.start()
    return order, copies


def states_kernel(nz, k_hbm, v_hbm, q_hbm, g_hbm, k, v, q, g, qc, c, early, late, *rest):
    pieces, sem = rest[:nz], rest[nz]
    order, copies = fetch(nz, (k_hbm, v_hbm, q_hbm, g_hbm), (k, v, q, g), sem)
    rows = q.shape[1]
    half = rows // 2
    per = q.shape[0] // nz
    block = lax.axis_index("major") * nz + lax.axis_index("minor")
    pos = block * rows + lax.broadcasted_iota(jnp.int32, (rows, LANES), 0)
    c[...] = 1.0 / jnp.sqrt(pos.astype(F32) + 1.0)
    for n in order:
        for copy in copies[n]:
            copy.wait()
        s_a = packed(tn(k[n, :half], v[n, :half]))
        s_b = packed(tn(k[n, half:], v[n, half:]))
        qc[n] = (q[n].astype(F32) * c[...]).astype(BF16)
        r_a = packed(tn(qc[n, :half], g[n, :half]))
        r_b = packed(tn(qc[n, half:], g[n, half:]))
        early[n] = s_a
        late[n] = r_b
        pieces[n // per][n % per, 0] = s_a + s_b
        pieces[n // per][n % per, 1] = r_a + r_b


def turned(w):
    n = w.shape[0]
    return jnp.concatenate([w[:, :n].T, w[:, n:].T], 1)


def inner_kernel(first, count, k, v, q, g, qc, c, early, late, o_att, o_gq, o_gk, o_gv):
    n = k.shape[1] // 2
    row = lax.broadcasted_iota(jnp.int32, (n, 2 * n), 0)
    col = jnp.bitwise_and(lax.broadcasted_iota(jnp.int32, (n, 2 * n), 1), n - 1)
    lower = row >= col
    for step in range(count):
        p = first + step
        s_bd = stacked(early[p].astype(BF16))
        r_bd = stacked(late[p].astype(BF16))
        for h in range(2):
            at = slice(h * n, (h + 1) * n)
            gc = (g[p, at].astype(F32) * c[at]).astype(BF16)
            ks, vs, gs, qs = map(stacked, (k[p, at], v[p, at], gc, qc[p, at]))
            w = jnp.where(lower, nt(q[p, at], ks), 0.0).astype(BF16)
            b = jnp.where(lower, nt(g[p, at], vs), 0.0).astype(BF16)
            att = nn(w, vs)
            gq = nn(b, ks)
            gv = nn(turned(w), gs)
            gk = nn(turned(b), qs)
            if h == 1:
                att = att + nn(q[p, at], s_bd)
                gq = gq + nt(g[p, at], s_bd)
            else:
                gk = gk + nt(v[p, at], r_bd)
                gv = gv + nn(k[p, at], r_bd)
            o_att[step, at] = att
            o_gq[step, at] = gq
            o_gk[step, at] = gk
            o_gv[step, at] = gv


def totals_kernel(nz, *refs):
    total = refs[0][...]
    for s in range(1, nz):
        total = total + refs[s][...]
    refs[nz][...] = total


def column_kernel(peers, last, t, t_other, *out):
    major = lax.axis_index("major")
    core = jnp.bitwise_and(major, 1)
    column = t[...] + t_other[...]
    for ref, masks in zip(out, peers):
        there = jnp.bitwise_xor(major, jnp.where(core == 0, masks[0], masks[1]))
        ref[...] = jnp.where(there > major, column[:, 0], column[:, 1])
    there = jnp.bitwise_xor(major, last)
    n = HD // 2
    chosen = jnp.where(there > major, column[:, 0], column[:, 1])
    out[-1][...] = jnp.where(core == 0, chosen[:, :n], chosen[:, n:])


def offsets_kernel(peers, last, *refs):
    out = refs[-1]
    major = lax.axis_index("major")
    core = jnp.bitwise_and(major, 1)
    from_last = refs[len(peers)][...]
    zero = jnp.zeros_like(from_last)
    total = jnp.concatenate(
        [jnp.where(core == 0, from_last, zero), jnp.where(core == 0, zero, from_last)], 1
    )
    earlier = jnp.bitwise_xor(major, last) < major
    s = jnp.where(earlier, total, 0.0)
    r = jnp.where(earlier, 0.0, total)
    for ref, masks in zip(refs, peers):
        earlier = jnp.bitwise_xor(major, jnp.where(core == 0, masks[0], masks[1])) < major
        s = s + jnp.where(earlier, ref[...], 0.0)
        r = r + jnp.where(earlier, 0.0, ref[...])
    out[:, 0] = s
    out[:, 1] = r


def prefixes_kernel(nz, *refs):
    raw, (t_other, x_own, x_other), out = refs[:nz], refs[nz:nz + 3], refs[nz + 3:]
    core = jnp.bitwise_and(lax.axis_index("major"), 1)
    z = lax.axis_index("minor")
    for kind in range(2):
        base = x_own[:, kind] + x_other[:, kind]
        base = base + jnp.where(core == 1 - kind, t_other[:, kind], 0.0)
        for slot in range(nz):
            there = jnp.bitwise_xor(z, slot)
            total = base
            for s in range(nz):
                if s == slot:
                    continue
                source = jnp.bitwise_xor(z, s)
                counts = source < there if kind == 0 else source > there
                total = total + jnp.where(counts, raw[s][:, kind], 0.0)
            out[kind * nz + slot][...] = total


def outer_kernel(kind, nz, cuts, *refs):
    parts = len(cuts) - 1
    x, y, c = refs[:3]
    inner = refs[3:3 + 2 * parts]
    pieces = refs[3 + 2 * parts:3 + 2 * parts + nz]
    out_x, out_y, *flag, stage, sem = refs[3 + 2 * parts + nz:]
    for ref in flag:
        ref[...] = jnp.zeros_like(ref)
    per = x.shape[0] // nz
    z = lax.axis_index("minor")
    copies = []
    for n in range(x.shape[0]):
        slot, i = divmod(n, per)
        p = jnp.bitwise_xor(z, slot) * per + i
        lanes = pl.ds(pl.multiple_of(p * LANES, LANES), LANES)
        state = stacked(pieces[slot][i].astype(BF16))
        part = max(j for j in range(parts) if cuts[j] <= n)
        own = [ref[n - cuts[part]] for ref in inner[2 * part:2 * part + 2]]
        first = own[0] + nn(x[n], state)
        second = own[1] + nt(y[n], state)
        if kind == 0:
            first = first * c[...]
            second = second * c[...]
        for a, (result, out) in enumerate(((first, out_x), (second, out_y))):
            stage[a, n] = result.astype(BF16)
            copy = pltpu.make_async_copy(stage.at[a, n], out.at[:, lanes], sem.at[a, n])
            copy.start()
            copies.append(copy)
    for copy in copies:
        copy.wait()


class Chain:
    def __init__(self):
        self.after = ()

    def __call__(self, body, outs, ins, n_hbm=0, scratch=(), mib=8, flops=0, name=None):
        n_in, n_after = len(ins), len(self.after)

        def kernel(*refs):
            body(*refs[:n_in], *refs[n_in + n_after:])

        result = pl.pallas_call(
            kernel,
            out_shape=tuple(o if hasattr(o, "shape") else pltpu.VMEM(*o) for o in outs),
            in_specs=[ANY] * n_hbm + [VM] * (n_in - n_hbm + n_after),
            out_specs=tuple(ANY if hasattr(o, "shape") else VM for o in outs),
            scratch_shapes=scratch,
            compiler_params=pltpu.CompilerParams(vmem_limit_bytes=mib * 2**20),
            cost_estimate=pl.CostEstimate(flops=flops, transcendentals=0, bytes_accessed=0),
            name=name,
        )(*ins, *self.after)
        self.after = (result[-1],)
        return result


def xor(count, even, odd=None):
    return [(i, i ^ (odd if odd is not None and i & 1 else even)) for i in range(count)]


def spread(own, nz):
    out = [own[0]] + [None] * (nz - 1)
    for s in range(nz - 1, 0, -1):
        out[s] = lax.ppermute(own[s], "minor", xor(nz, s))
    return out


def on_device(queries, keys, values, cotangent):
    rows, columns = queries.shape
    pairs = columns // LANES
    nz, nm = lax.axis_size("minor"), lax.axis_size("major")
    per = pairs // nz
    plane = ((pairs, rows, LANES), BF16)
    both = ((per, 2, HD, LANES), F32)
    piece = ((per, HD, LANES), F32)
    half_piece = ((per, HD // 2, LANES), F32)
    state = ((pairs, HD, LANES), F32)
    masks = list(range(2, nm, 2))
    last = masks.pop()
    peers = list(zip(masks[0::2], masks[1::2]))
    run = Chain()

    k, v, q, g, qc, c, early, late, *mine = run(
        functools.partial(states_kernel, nz),
        [plane] * 5 + [((rows, LANES), F32), state, state] + [both] * nz,
        [pltpu.with_memory_space_constraint(x, pltpu.HBM) for x in (keys, values, queries, cotangent)],
        n_hbm=4, scratch=[pltpu.SemaphoreType.DMA((4, pairs))], name="states",
    )
    raw = spread(mine, nz)
    cuts = [n * pairs // 8 for n in CUTS]
    inner = []

    def work():
        n = len(inner)
        first, count = cuts[n], cuts[n + 1] - cuts[n]
        inner.append(run(
            functools.partial(inner_kernel, first, count), [((count, rows, LANES), F32)] * 4,
            (k, v, q, g, qc, c, early, late), mib=16, flops=count * 5 * 10**8, name="inner",
        ))

    work()
    (t,) = run(functools.partial(totals_kernel, nz), [both], raw, name="totals")
    t_other = lax.ppermute(t, "major", xor(nm, 1))
    sent = run(
        functools.partial(column_kernel, peers, last), [piece] * len(peers) + [half_piece],
        (t, t_other), name="column",
    )
    there = [lax.ppermute(x, "major", xor(nm, *m)) for x, m in zip(sent, peers)]
    there.append(lax.ppermute(sent[-1], "major", xor(nm, last)))
    (x,) = run(functools.partial(offsets_kernel, peers, last), [both], there, name="offsets")
    x_other = lax.ppermute(x, "major", xor(nm, 1))
    ready = run(
        functools.partial(prefixes_kernel, nz), [piece] * (2 * nz), (*raw, t_other, x, x_other),
        name="prefixes",
    )
    s_in = spread(ready[:nz], nz)
    r_in = spread(ready[nz:], nz)
    work()

    def outer(kind, x, y, which, pieces, flag=()):
        parts = [part[a] for part in inner for a in which]
        out = jax.ShapeDtypeStruct((rows, columns), BF16)
        return run(
            functools.partial(outer_kernel, kind, nz, cuts), (out, out, *flag),
            (x, y, c, *parts, *pieces),
            scratch=[pltpu.VMEM((2, pairs, rows, LANES), BF16), pltpu.SemaphoreType.DMA((2, pairs))],
            mib=12, flops=10**8, name="outer",
        )

    attended, grad_q, _ = outer(0, q, g, (0, 1), s_in, [((8, LANES), F32)])
    grad_v, grad_k = outer(1, k, v, (3, 2), r_in)
    return attended, grad_q, grad_k, grad_v


def solution(mesh):
    spec = P(("major", "minor"), None)
    return jax.shard_map(
        on_device, mesh=mesh, in_specs=(spec,) * 4, out_specs=(spec,) * 4, check_vma=False
    )
```

```python
import functools

import jax
import jax.numpy as jnp
from jax import lax
from jax.experimental import pallas as pl
from jax.experimental.pallas import tpu as pltpu
from jax.sharding import PartitionSpec as P

HD = 64
LANES = 2 * HD
F32 = jnp.float32
BF16 = jnp.bfloat16
CUTS = (0, 5, 8)


VM = pl.BlockSpec(memory_space=pltpu.VMEM)
ANY = pl.BlockSpec(memory_space=pltpu.HBM)


def dot(a, b, dims):
    return lax.dot_general(a, b, (dims, ((), ())), preferred_element_type=F32)


def nn(a, b):
    return dot(a, b, ((1,), (0,)))


def nt(a, b):
    return dot(a, b, ((1,), (1,)))


def tn(a, b):
    return dot(a, b, ((0,), (0,)))


def first_head(shape):
    return lax.broadcasted_iota(jnp.int32, shape, len(shape) - 1) < HD


def stacked(x):
    first = first_head(x.shape)
    zero = jnp.zeros_like(x)
    return jnp.concatenate([jnp.where(first, x, zero), jnp.where(first, zero, x)], 0)


def packed(m):
    return jnp.where(first_head((HD, LANES)), m[:HD], m[HD:])


def fetch(nz, sources, planes, sem):
    per = planes[0].shape[0] // nz
    z = lax.axis_index("minor")
    order = [slot * per + i for slot in range(nz - 1, -1, -1) for i in range(per)]
    copies = {}
    for n in order:
        p = jnp.bitwise_xor(z, n // per) * per + n % per
        lanes = pl.ds(pl.multiple_of(p * LANES, LANES), LANES)
        copies[n] = [
            pltpu.make_async_copy(src.at[:, lanes], dst.at[n], sem.at[a, n])
            for a, (src, dst) in enumerate(zip(sources, planes))
        ]
        for copy in copies[n]:
            copy.start()
    return order, copies


def states_kernel(nz, k_hbm, v_hbm, q_hbm, g_hbm, k, v, q, g, qc, c, early, late, *rest):
    pieces, sem = rest[:nz], rest[nz]
    order, copies = fetch(nz, (k_hbm, v_hbm, q_hbm, g_hbm), (k, v, q, g), sem)
    rows = q.shape[1]
    half = rows // 2
    per = q.shape[0] // nz
    block = lax.axis_index("major") * nz + lax.axis_index("minor")
    pos = block * rows + lax.broadcasted_iota(jnp.int32, (rows, LANES), 0)
    c[...] = 1.0 / jnp.sqrt(pos.astype(F32) + 1.0)
    def states(x, y, ns, at):
        m = tn(*(jnp.concatenate([ref[n, at] for n in ns], 1) for ref in (x, y)))
        return [packed(m[i * LANES:(i + 1) * LANES, i * LANES:(i + 1) * LANES]) for i in range(len(ns))]

    halves = slice(0, half), slice(half, rows)
    for ns in (order[i:i + 2] for i in range(0, len(order), 2)):
        for n in ns:
            for copy in copies[n]:
                copy.wait()
            qc[n] = (q[n].astype(F32) * c[...]).astype(BF16)
        s_a, s_b = (states(k, v, ns, at) for at in halves)
        r_a, r_b = (states(qc, g, ns, at) for at in halves)
        for i, n in enumerate(ns):
            early[n] = s_a[i]
            late[n] = r_b[i]
            pieces[n // per][n % per, 0] = s_a[i] + s_b[i]
            pieces[n // per][n % per, 1] = r_a[i] + r_b[i]


def turned(w):
    n = w.shape[0]
    return jnp.concatenate([w[:, :n].T, w[:, n:].T], 1)


def inner_kernel(first, count, k, v, q, g, qc, c, early, late, o_att, o_gq, o_gk, o_gv):
    n = k.shape[1] // 2
    row = lax.broadcasted_iota(jnp.int32, (n, 2 * n), 0)
    col = jnp.bitwise_and(lax.broadcasted_iota(jnp.int32, (n, 2 * n), 1), n - 1)
    lower = row >= col
    for step in range(count):
        p = first + step
        s_bd = stacked(early[p].astype(BF16))
        r_bd = stacked(late[p].astype(BF16))
        for h in range(2):
            at = slice(h * n, (h + 1) * n)
            gc = (g[p, at].astype(F32) * c[at]).astype(BF16)
            ks, vs, gs, qs = map(stacked, (k[p, at], v[p, at], gc, qc[p, at]))
            w = jnp.where(lower, nt(q[p, at], ks), 0.0).astype(BF16)
            b = jnp.where(lower, nt(g[p, at], vs), 0.0).astype(BF16)
            att = nn(w, vs)
            gq = nn(b, ks)
            gv = nn(turned(w), gs)
            gk = nn(turned(b), qs)
            if h == 1:
                att = att + nn(q[p, at], s_bd)
                gq = gq + nt(g[p, at], s_bd)
            else:
                gk = gk + nt(v[p, at], r_bd)
                gv = gv + nn(k[p, at], r_bd)
            o_att[step, at] = att
            o_gq[step, at] = gq
            o_gk[step, at] = gk
            o_gv[step, at] = gv


def totals_kernel(nz, *refs):
    total = refs[0][...]
    for s in range(1, nz):
        total = total + refs[s][...]
    refs[nz][...] = total


def column_kernel(peers, last, t, t_other, *out):
    major = lax.axis_index("major")
    core = jnp.bitwise_and(major, 1)
    column = t[...] + t_other[...]
    for ref, masks in zip(out, peers):
        there = jnp.bitwise_xor(major, jnp.where(core == 0, masks[0], masks[1]))
        ref[...] = jnp.where(there > major, column[:, 0], column[:, 1])
    there = jnp.bitwise_xor(major, last)
    n = HD // 2
    chosen = jnp.where(there > major, column[:, 0], column[:, 1])
    out[-1][...] = jnp.where(core == 0, chosen[:, :n], chosen[:, n:])


def offsets_kernel(peers, last, *refs):
    out = refs[-1]
    major = lax.axis_index("major")
    core = jnp.bitwise_and(major, 1)
    from_last = refs[len(peers)][...]
    zero = jnp.zeros_like(from_last)
    total = jnp.concatenate(
        [jnp.where(core == 0, from_last, zero), jnp.where(core == 0, zero, from_last)], 1
    )
    earlier = jnp.bitwise_xor(major, last) < major
    s = jnp.where(earlier, total, 0.0)
    r = jnp.where(earlier, 0.0, total)
    for ref, masks in zip(refs, peers):
        earlier = jnp.bitwise_xor(major, jnp.where(core == 0, masks[0], masks[1])) < major
        s = s + jnp.where(earlier, ref[...], 0.0)
        r = r + jnp.where(earlier, 0.0, ref[...])
    out[:, 0] = s
    out[:, 1] = r


def prefixes_kernel(nz, *refs):
    raw, (t_other, x_own, x_other), out = refs[:nz], refs[nz:nz + 3], refs[nz + 3:]
    core = jnp.bitwise_and(lax.axis_index("major"), 1)
    z = lax.axis_index("minor")
    for kind in range(2):
        base = x_own[:, kind] + x_other[:, kind]
        base = base + jnp.where(core == 1 - kind, t_other[:, kind], 0.0)
        for slot in range(nz):
            there = jnp.bitwise_xor(z, slot)
            total = base
            for s in range(nz):
                if s == slot:
                    continue
                source = jnp.bitwise_xor(z, s)
                counts = source < there if kind == 0 else source > there
                total = total + jnp.where(counts, raw[s][:, kind], 0.0)
            out[slot][:, kind] = total


def outer_kernel(nz, cuts, *refs):
    parts = len(cuts) - 1
    q, k, v, g, c = refs[:5]
    inner = refs[5:5 + 4 * parts]
    pieces = refs[5 + 4 * parts:5 + 4 * parts + nz]
    outs = refs[5 + 4 * parts + nz:9 + 4 * parts + nz]
    stage, sem = refs[9 + 4 * parts + nz:]
    per = q.shape[0] // nz
    z = lax.axis_index("minor")
    copies = []
    for n in range(q.shape[0]):
        slot, i = divmod(n, per)
        p = jnp.bitwise_xor(z, slot) * per + i
        lanes = pl.ds(pl.multiple_of(p * LANES, LANES), LANES)
        s_bd = stacked(pieces[slot][i, 0].astype(BF16))
        r_bd = stacked(pieces[slot][i, 1].astype(BF16))
        part = max(j for j in range(parts) if cuts[j] <= n)
        own = [ref[n - cuts[part]] for ref in inner[4 * part:4 * part + 4]]
        scale = c[...]
        results = (
            (own[0] + nn(q[n], s_bd)) * scale,
            (own[1] + nt(g[n], s_bd)) * scale,
            own[2] + nt(v[n], r_bd),
            own[3] + nn(k[n], r_bd),
        )
        for a, result in enumerate(results):
            stage[a, n] = result.astype(BF16)
            copy = pltpu.make_async_copy(stage.at[a, n], outs[a].at[:, lanes], sem.at[a, n])
            copy.start()
            copies.append(copy)
    for copy in copies:
        copy.wait()


class Chain:
    def __init__(self):
        self.after = ()

    def __call__(self, body, outs, ins, n_hbm=0, scratch=(), mib=8, flops=0, name=None):
        n_in, n_after = len(ins), len(self.after)

        def kernel(*refs):
            body(*refs[:n_in], *refs[n_in + n_after:])

        result = pl.pallas_call(
            kernel,
            out_shape=tuple(o if hasattr(o, "shape") else pltpu.VMEM(*o) for o in outs),
            in_specs=[ANY] * n_hbm + [VM] * (n_in - n_hbm + n_after),
            out_specs=tuple(ANY if hasattr(o, "shape") else VM for o in outs),
            scratch_shapes=scratch,
            compiler_params=pltpu.CompilerParams(vmem_limit_bytes=mib * 2**20),
            cost_estimate=pl.CostEstimate(flops=flops, transcendentals=0, bytes_accessed=0),
            name=name,
        )(*ins, *self.after)
        self.after = (result[-1],)
        return result


def xor(count, even, odd=None):
    return [(i, i ^ (odd if odd is not None and i & 1 else even)) for i in range(count)]


def spread(own, nz):
    out = [own[0]] + [None] * (nz - 1)
    for s in range(nz - 1, 0, -1):
        out[s] = lax.ppermute(own[s], "minor", xor(nz, s))
    return out


def on_device(queries, keys, values, cotangent):
    rows, columns = queries.shape
    pairs = columns // LANES
    nz, nm = lax.axis_size("minor"), lax.axis_size("major")
    per = pairs // nz
    plane = ((pairs, rows, LANES), BF16)
    both = ((per, 2, HD, LANES), F32)
    piece = ((per, HD, LANES), F32)
    half_piece = ((per, HD // 2, LANES), F32)
    state = ((pairs, HD, LANES), F32)
    masks = list(range(2, nm, 2))
    last = masks.pop()
    peers = list(zip(masks[0::2], masks[1::2]))
    run = Chain()

    k, v, q, g, qc, c, early, late, *mine = run(
        functools.partial(states_kernel, nz),
        [plane] * 5 + [((rows, LANES), F32), state, state] + [both] * nz,
        [pltpu.with_memory_space_constraint(x, pltpu.HBM) for x in (keys, values, queries, cotangent)],
        n_hbm=4, scratch=[pltpu.SemaphoreType.DMA((4, pairs))], name="states",
    )
    raw = spread(mine, nz)
    cuts = [n * pairs // 8 for n in CUTS]
    inner = []

    def work():
        n = len(inner)
        first, count = cuts[n], cuts[n + 1] - cuts[n]
        inner.append(run(
            functools.partial(inner_kernel, first, count), [((count, rows, LANES), F32)] * 4,
            (k, v, q, g, qc, c, early, late), mib=16, flops=count * 5 * 10**8, name="inner",
        ))

    work()
    (t,) = run(functools.partial(totals_kernel, nz), [both], raw, name="totals")
    t_other = lax.ppermute(t, "major", xor(nm, 1))
    sent = run(
        functools.partial(column_kernel, peers, last), [piece] * len(peers) + [half_piece],
        (t, t_other), name="column",
    )
    diagonal = lax.ppermute(sent[-1], "major", xor(nm, last))
    there = [lax.ppermute(x, "major", xor(nm, *m)) for x, m in zip(sent, peers)]
    there.append(diagonal)
    (x,) = run(functools.partial(offsets_kernel, peers, last), [both], there, name="offsets")
    x_other = lax.ppermute(x, "major", xor(nm, 1))
    ready = run(
        functools.partial(prefixes_kernel, nz), [both] * nz, (*raw, t_other, x, x_other),
        name="prefixes",
    )
    state_in = spread(ready, nz)
    work()

    out = jax.ShapeDtypeStruct((rows, columns), BF16)
    return run(
        functools.partial(outer_kernel, nz, cuts), (out,) * 4,
        (q, k, v, g, c, *[x for part in inner for x in part], *state_in),
        scratch=[pltpu.VMEM((4, pairs, rows, LANES), BF16), pltpu.SemaphoreType.DMA((4, pairs))],
        mib=12, flops=10**8, name="outer",
    )


def solution(mesh):
    spec = P(("major", "minor"), None)
    return jax.shard_map(
        on_device, mesh=mesh, in_specs=(spec,) * 4, out_specs=(spec,) * 4, check_vma=False
    )
```
